32 devices in a mesh: ends: 2 (over x), dp: 4 (over y, core), tp: 4 (over z).
Axes of the slice: x: 2, y: 2, z: 4, core: 2. Of those that a mesh axis runs over, the one named last changes fastest.
Arguments:
- grad: bfloat16 [2, 4, 4096, 3072], P('ends', 'dp', 'tp'), may hold values from -1800 to 1800
- master: float32 [4, 1024, 3072], P('tp', ('ends', 'dp')), may hold values from -3 to 3
- moment: float32 [4, 1024, 3072], P('tp', ('ends', 'dp')), may hold values from -3 to 3
- second: float32 [4, 1024, 3072], P('tp', ('ends', 'dp')), may hold values from 0.01 to 1
Outputs:
- weights: bfloat16 [4096, 3072], P('tp')
- master_out: float32 [4, 1024, 3072], P('tp', ('ends', 'dp'))
- moment_out: float32 [4, 1024, 3072], P('tp', ('ends', 'dp'))
- second_out: float32 [4, 1024, 3072], P('tp', ('ends', 'dp'))
The draws below stay inside these ranges and needn't reach their ends.
All inputs are finite; a program needn't handle non-finite values.
Results may differ from the reference program's by a relative error of at most 0.0034.
Values may be sent and summed in bfloat16 or wider, within the bound.
A program may use at most 128 MiB of HBM per device.

```python
import math
import jax
import jax.numpy as jnp
from jax import lax

D = 3072
STEP = 10
ROWS_TP = 1024
VOCAB = 4096
N_ENDS = 2
N_DP = 4
N_TP = 4


def draw_grad(key, part):
    keys = jax.random.split(jax.random.fold_in(key, 17), 4)
    shape = (N_ENDS, N_DP, VOCAB, D)
    base = jax.random.truncated_normal(keys[0], -4.0, 4.0, shape, jnp.float32)
    members = N_ENDS * N_DP
    member = 0.5 * 3.0 ** (jnp.arange(members, dtype=jnp.float32) / max(members - 1, 1))
    member = member.reshape(N_ENDS, N_DP, 1, 1)
    position = (jnp.arange(VOCAB, dtype=jnp.int32) % ROWS_TP).astype(jnp.float32) / ROWS_TP
    rough = jnp.exp(jax.random.uniform(keys[2], (VOCAB,), jnp.float32, 0.0, math.log(10.0)))
    row_scale = 3.0 ** position * rough
    col_scale = jnp.exp(jax.random.uniform(keys[3], (D,), jnp.float32, 0.0, math.log(10.0)))
    values = base * member * row_scale[None, None, :, None] * col_scale[None, None, None, :]
    return values.astype(jnp.bfloat16)


def block_scale(stream_key, extent, shards, low, largest):
    gain, own = 1.0, jax.random.fold_in(stream_key, 6)
    for axis_at, parts in shards:
        draws = jnp.exp(jax.random.uniform(jax.random.fold_in(own, axis_at), (parts,), jnp.float32, low / len(shards), largest / len(shards)))
        gain = gain * jnp.repeat(draws, extent[axis_at] // parts).reshape([-1 if axis == axis_at else 1 for axis in range(len(extent))])
    return gain


def scatter_about(key, extent, deviation, most, pieces=(), held_as=jnp.bfloat16):
    result = jax.random.normal(key, extent, jnp.float32) * deviation
    if len(pieces) > 0:
        result = block_scale(key, extent, pieces, -0.22, 0.18) * result
    return jnp.clip(result, min=-most, max=most).astype(held_as)


def setup_inputs(seed: int = 0) -> dict:
    streams_of = jax.random.split(jax.random.key(seed), 5)
    return {
        "grad": draw_grad(jax.random.fold_in(streams_of[4], 71), 0),
        "master": scatter_about(streams_of[1], (N_TP, ROWS_TP, D), 0.5, 3.0, ((0, 4), (1, 8)), jnp.float32),
        "moment": scatter_about(streams_of[2], (N_TP, ROWS_TP, D), 0.5, 3.0, ((0, 4), (1, 8)), jnp.float32),
        "second": jnp.clip(jnp.exp(math.log(1.0) - 4.6051702 * jax.random.uniform(streams_of[3], (N_TP, ROWS_TP, D), jnp.float32) ** block_scale(streams_of[3], (N_TP, ROWS_TP, D), ((0, 4), (1, 8)), -0.2, 0.2)), 0.01, 1.0),
    }


def reference(grad, master, moment, second):
    stacked = grad.reshape(N_ENDS * N_DP, VOCAB, D)

    def accumulate(carry, member):
        return (carry + member.astype(jnp.float32), None)
    summed, _ = lax.scan(accumulate, jnp.zeros((VOCAB, D), jnp.float32), stacked)
    norm = jnp.sqrt(jnp.sum(summed * summed))
    factor = jnp.minimum(jnp.float32(1.0), jnp.sqrt(jnp.float32(VOCAB * D)) / (norm + 1e-06))
    clipped = (factor * summed).reshape(N_TP, ROWS_TP, D)
    moment_out = 0.9 * moment + 0.1 * clipped
    second_out = 0.999 * second + 0.001 * clipped * clipped
    update = moment_out / (1.0 - 0.9 ** STEP) / (jnp.sqrt(second_out / (1.0 - 0.999 ** STEP)) + 1e-08)
    master_out = master - 0.01 * (update + 0.1 * master)
    weights = master_out.reshape(VOCAB, D).astype(jnp.bfloat16)
    return (weights, master_out, moment_out, second_out)
```

```python
import functools
import math

import jax
import jax.numpy as jnp
from jax import lax
from jax.experimental import pallas as pl
from jax.experimental.pallas import tpu as pltpu
from jax.sharding import PartitionSpec as P

STEP = 10
MESH = pl.DeviceIdType.MESH
F32 = jnp.float32
BF16 = jnp.bfloat16


def remote(src, dst, send, recv, device):
    return pltpu.make_async_remote_copy(
        src_ref=src, dst_ref=dst, send_sem=send, recv_sem=recv, device_id=device, device_id_type=MESH
    )


def kernel(cfg, grad, master, moment, second, w_out, master_out, moment_out, second_out, *scratch):
    ends, ys, tps, rows, width, pieces, staged = cfg
    if staged:
        w_hbm, (w_out, w_sem), scratch = w_out, scratch[-2:], scratch[:-2]
    (own, peer, part1, land1, part2, land2, total, st0, st1, st2, squares,
     own_sem, st_sem, peer_s, peer_r, s1, r1, s2, r2, ns, nr, a_s, a_r, b_s, b_r, f_s, f_r, p_s, p_r) = scratch
    e, dp, t = lax.axis_index("ends"), lax.axis_index("dp"), lax.axis_index("tp")
    y, c = dp // 2, lax.rem(dp, 2)
    ch = rows // pieces
    devices = ends * ys * 2 * tps
    square = ends == ys
    n1, n2 = (ends, ys) if square else (ys, ends)

    def place(core, da, db):
        if square:
            ends_first = core == 0
            de, dy = jnp.where(ends_first, da, db), jnp.where(ends_first, db, da)
        else:
            de, dy = db, da
        return lax.rem(e + de, ends), lax.rem(y + dy, ys)

    def first_row(core, da, db):
        ee, yy = place(core, da, db)
        return pl.multiple_of(((ee * ys + yy) * 2 + core) * rows, rows)

    def at(da, db):
        ee, yy = place(c, da, db)
        return {"ends": ee, "dp": yy * 2 + c}

    partner = {"dp": y * 2 + (1 - c)}
    shifts1, shifts2 = range(1, n1), range(1, n2)
    order = (
        [(da, db) for da in shifts1 for db in shifts2]
        + [(0, db) for db in shifts2]
        + [(da, 0) for da in shifts1]
        + [(0, 0)]
    )
    slot = lambda da, db: da * n2 + db
    part = lambda k: pl.ds(k * ch, ch)

    def own_copy(da, db, k):
        i = slot(da, db)
        r = pl.multiple_of(first_row(c, da, db) + k * ch, ch)
        return pltpu.make_async_copy(grad.at[pl.ds(r, ch)], own.at[i, part(k)], own_sem.at[i * pieces + k])

    for da, db in order:
        for k in range(pieces):
            own_copy(da, db, k).start()
    state_copies = [
        pltpu.make_async_copy(src, dst, st_sem.at[i])
        for i, (src, dst) in enumerate(((master, st0), (moment, st1), (second, st2)))
    ]

    me = (e * (ys * 2) + dp) * tps + t

    def device_of(i):
        return {"ends": i // (ys * 2 * tps), "dp": lax.rem(i // tps, ys * 2), "tp": lax.rem(i, tps)}

    barrier = pltpu.get_barrier_semaphore()

    @pl.loop(1, devices)
    def _(d):
        pl.semaphore_signal(barrier, inc=1, device_id=device_of(lax.rem(me + d, devices)), device_id_type=MESH)

    pl.semaphore_wait(barrier, devices - 1)

    for da, db in order:
        for k in range(pieces):
            i = slot(da, db)
            r = pl.multiple_of(first_row(1 - c, da, db) + k * ch, ch)
            remote(grad.at[pl.ds(r, ch)], peer.at[i, part(k)], peer_s, peer_r.at[i * pieces + k], partner).start()
    for copy in state_copies:
        copy.start()

    def chip_sum(da, db, k):
        i = slot(da, db)
        own_copy(da, db, k).wait()
        remote(peer.at[i, part(k)], peer.at[i, part(k)], peer_s, peer_r.at[i * pieces + k], partner).wait_recv()
        return own[i, part(k), :].astype(F32) + peer[i, part(k), :].astype(F32)

    def copy1(da, db, k):
        i = (da - 1) * n2 + db
        return remote(part1.at[i, part(k)], land1.at[i, part(k)], s1, r1.at[i * pieces + k], at(da, 0))

    def copy2(db, k):
        i = db - 1
        return remote(part2.at[i, part(k)], land2.at[i, part(k)], s2, r2.at[i * pieces + k], at(0, db))

    def send1(da, db, k):
        part1[(da - 1) * n2 + db, part(k), :] = chip_sum(da, db, k).astype(BF16)
        copy1(da, db, k).start()

    def sum1(db, k):
        value = chip_sum(0, db, k)
        for da in shifts1:
            copy1(da, db, k).wait_recv()
            value = value + land1[(da - 1) * n2 + db, part(k), :].astype(F32)
        return value

    for k in range(pieces):
        for da in shifts1:
            for db in shifts2:
                send1(da, db, k)
    for k in range(pieces):
        for da in shifts1:
            send1(da, 0, k)
        for db in shifts2:
            part2[db - 1, part(k), :] = sum1(db, k).astype(BF16)
            copy2(db, k).start()
    acc = jnp.zeros((8, width), F32)
    for k in range(pieces):
        value = sum1(0, k)
        for db in shifts2:
            copy2(db, k).wait_recv()
            value = value + land2[db - 1, part(k), :].astype(F32)
        total[part(k), :] = value
        value = value * value
        for r in range(0, ch, 8):
            acc = acc + value[r : r + 8, :]

    mine = acc[:, :128]
    for j in range(128, width, 128):
        mine = mine + acc[:, j : j + 128]
    squares[me] = mine

    @pl.loop(1, devices)
    def _(d):
        remote(squares.at[me], squares.at[me], ns, nr, device_of(lax.rem(me + d, devices))).start()

    others = squares.at[pl.ds(0, devices - 1)]
    everyone = remote(others, others, ns, nr, partner)
    for copy in state_copies:
        copy.wait()
    everyone.wait_recv()
    everyone.wait_send()
    norm2 = jnp.full((8, 128), jnp.sum(jnp.sum(squares[...], axis=0)), F32)
    entries = float(tps * ends * ys * 2 * rows * width)
    factor = jnp.minimum(F32(1.0), F32(math.sqrt(entries)) / (jnp.sqrt(norm2) + 1e-06))[:1, :1]

    my_row = first_row(c, 0, 0)

    def piece_of(da, db, k):
        return w_out.at[pl.ds(pl.multiple_of(first_row(c, da, db) + k * ch, ch), ch)]

    def copy_a(da, src, k):
        return remote(src, src, a_s, a_r.at[(da - 1) * pieces + k], at(da, 0))

    def copy_b(db, src, k):
        return remote(src, src, b_s, b_r.at[(db - 1) * pieces + k], at(0, db))

    def copy_f(da, db, src, k):
        return remote(src, src, f_s, f_r.at[((da - 1) * (n2 - 1) + db - 1) * pieces + k], at(0, db))

    def copy_p(src):
        return remote(src, src, p_s, p_r, partner)

    for k in range(pieces):
        @pl.loop(0, ch // 16)
        def _(g):
            at_row = pl.multiple_of(k * ch + g * 16, 16)
            here = pl.ds(at_row, 16)
            clipped = factor * total[here, :]
            m = 0.9 * st1[here, :] + 0.1 * clipped
            v = 0.999 * st2[here, :] + 0.001 * clipped * clipped
            update = m / (1.0 - 0.9**STEP) / (jnp.sqrt(v / (1.0 - 0.999**STEP)) + 1e-08)
            w = st0[here, :]
            w = w - 0.01 * (update + 0.1 * w)
            moment_out[here, :] = m
            second_out[here, :] = v
            master_out[here, :] = w
            w_out[pl.ds(pl.multiple_of(my_row + at_row, 16), 16), :] = w.astype(BF16)

        src = piece_of(0, 0, k)
        for da in shifts1:
            copy_a(da, src, k).start()
        for db in shifts2:
            copy_b(db, src, k).start()
        copy_p(src).start()

    for k in range(pieces):
        for da in shifts1:
            src = piece_of(n1 - da, 0, k)
            copy_a(da, src, k).wait_recv()
            for db in shifts2:
                copy_f(da, db, src, k).start()
            copy_p(src).start()
        for db in shifts2:
            src = piece_of(0, n2 - db, k)
            copy_b(db, src, k).wait_recv()
            copy_p(src).start()
    for k in range(pieces):
        for da in shifts1:
            for db in shifts2:
                src = piece_of(n1 - da, n2 - db, k)
                copy_f(da, db, src, k).wait_recv()
                copy_p(src).start()

    half = w_out.at[pl.ds(0, n1 * n2 * rows)]
    remote(half, half, p_s, p_r, partner).wait_recv()
    remote(half, half, p_s, p_r, partner).wait_send()
    remote(peer, peer, peer_s, peer_r.at[0], partner).wait_send()
    remote(part1, land1, s1, r1.at[0], partner).wait_send()
    remote(part2, land2, s2, r2.at[0], partner).wait_send()
    for sem, count, recv in ((a_s, n1 - 1, a_r), (b_s, n2 - 1, b_r), (f_s, (n1 - 1) * (n2 - 1), f_r)):
        ref = w_out.at[pl.ds(0, count * rows)]
        remote(ref, ref, sem, recv.at[0], partner).wait_send()
    if staged:
        final = pltpu.make_async_copy(w_out, w_hbm, w_sem)
        final.start()
        final.wait()


def per_device(mesh, grad, master, moment, second):
    ends, dps, tps = (mesh.shape[name] for name in ("ends", "dp", "tp"))
    ys = dps // 2
    rows_tp, width = grad.shape[2:]
    rows = rows_tp // (ends * dps)
    pieces = 4 if rows % 64 == 0 else 1
    n1, n2 = (ends, ys) if ends == ys else (ys, ends)
    blocks = n1 * n2
    devices = ends * dps * tps
    dma = lambda n: pltpu.SemaphoreType.DMA((n,))
    one = pltpu.SemaphoreType.DMA
    block = lambda n, dtype=BF16: pltpu.VMEM((n, rows, width), dtype)
    state = lambda: pltpu.VMEM((rows, width), F32)
    scratch = [
        block(blocks), block(blocks),
        block((n1 - 1) * n2), block((n1 - 1) * n2),
        block(n2 - 1), block(n2 - 1),
        state(), state(), state(), state(),
        pltpu.VMEM((devices, 8, 128), F32),
        dma(blocks * pieces), dma(3), one, dma(blocks * pieces),
        one, dma((n1 - 1) * n2 * pieces), one, dma((n2 - 1) * pieces),
        one, one,
        one, dma((n1 - 1) * pieces), one, dma((n2 - 1) * pieces),
        one, dma((n1 - 1) * (n2 - 1) * pieces),
        one, one,
    ]
    block_bytes = rows * width * 2
    staged = rows_tp * width * 2 > 8 << 20
    if staged:
        scratch += [pltpu.VMEM((rows_tp, width), BF16), one]
    limit = block_bytes * (2 * blocks + 2 * (n1 - 1) * n2 + 2 * (n2 - 1) + 8 + staged * ends * dps) + devices * 4096 + (3 << 20)
    stays = pl.BlockSpec(memory_space=pltpu.HBM)
    vmem = pl.BlockSpec(memory_space=pltpu.VMEM)
    weights, master_out, moment_out, second_out = pl.pallas_call(
        functools.partial(kernel, (ends, ys, tps, rows, width, pieces, staged)),
        out_shape=(
            (pltpu.HBM if staged else pltpu.VMEM)((rows_tp, width), BF16),
            pltpu.VMEM((rows, width), F32),
            pltpu.VMEM((rows, width), F32),
            pltpu.VMEM((rows, width), F32),
        ),
        in_specs=[stays] * 4,
        out_specs=(stays if staged else vmem,) + (vmem,) * 3,
        scratch_shapes=scratch,
        compiler_params=pltpu.CompilerParams(collective_id=0, has_side_effects=True, vmem_limit_bytes=limit),
        name="sum_update_gather",
    )(*(pltpu.with_memory_space_constraint(x, pltpu.HBM) for x in (grad[0, 0], master[0], moment[0], second[0])))
    return (weights, master_out[None], moment_out[None], second_out[None])


def solution(mesh):
    rows = P("tp", ("ends", "dp"), None)
    return jax.shard_map(
        functools.partial(per_device, mesh),
        mesh=mesh,
        in_specs=(P("ends", "dp", "tp", None), rows, rows, rows),
        out_specs=(P("tp", None), rows, rows, rows),
        check_vma=False,
    )
```

```python
import functools
import math

import jax
import jax.numpy as jnp
from jax import lax
from jax.experimental import pallas as pl
from jax.experimental.pallas import tpu as pltpu
from jax.sharding import PartitionSpec as P

STEP = 10
MESH = pl.DeviceIdType.MESH
F32 = jnp.float32
BF16 = jnp.bfloat16


def remote(src, dst, send, recv, device):
    return pltpu.make_async_remote_copy(
        src_ref=src, dst_ref=dst, send_sem=send, recv_sem=recv, device_id=device, device_id_type=MESH
    )


def kernel(cfg, grad, master, moment, second, w_out, master_out, moment_out, second_out, *scratch):
    ends, ys, tps, rows, width, pieces, staged = cfg
    if staged:
        w_hbm, (w_out, w_sem), scratch = w_out, scratch[-2:], scratch[:-2]
    (own, peer, part1, land1, part2, land2, total, st0, st1, st2, squares,
     own_sem, st_sem, peer_s, peer_r, s1, r1, s2, r2, ns, nr, a_s, a_r, b_s, b_r, f_s, f_r, p_s, p_r) = scratch
    e, dp, t = lax.axis_index("ends"), lax.axis_index("dp"), lax.axis_index("tp")
    y, c = dp // 2, lax.rem(dp, 2)
    ch = rows // pieces
    devices = ends * ys * 2 * tps
    square = ends == ys
    n1, n2 = (ends, ys) if square else (ys, ends)

    def place(core, da, db):
        if square:
            ends_first = core == 0
            de, dy = jnp.where(ends_first, da, db), jnp.where(ends_first, db, da)
        else:
            de, dy = db, da
        return lax.rem(e + de, ends), lax.rem(y + dy, ys)

    def first_row(core, da, db):
        ee, yy = place(core, da, db)
        return pl.multiple_of(((ee * ys + yy) * 2 + core) * rows, rows)

    def at(da, db):
        ee, yy = place(c, da, db)
        return {"ends": ee, "dp": yy * 2 + c}

    partner = {"dp": y * 2 + (1 - c)}
    shifts1, shifts2 = range(1, n1), range(1, n2)
    order = (
        [(da, db) for da in shifts1 for db in shifts2]
        + [(0, db) for db in shifts2]
        + [(da, 0) for da in shifts1]
        + [(0, 0)]
    )
    slot = lambda da, db: da * n2 + db
    part = lambda k: pl.ds(k * ch, ch)

    def own_copy(da, db, k):
        i = slot(da, db)
        r = pl.multiple_of(first_row(c, da, db) + k * ch, ch)
        return pltpu.make_async_copy(grad.at[pl.ds(r, ch)], own.at[i, part(k)], own_sem.at[i * pieces + k])

    for da, db in order:
        for k in range(pieces):
            own_copy(da, db, k).start()
    state_copies = [
        pltpu.make_async_copy(src, dst, st_sem.at[i])
        for i, (src, dst) in enumerate(((master, st0), (moment, st1), (second, st2)))
    ]

    me = (e * (ys * 2) + dp) * tps + t

    def device_of(i):
        return {"ends": i // (ys * 2 * tps), "dp": lax.rem(i // tps, ys * 2), "tp": lax.rem(i, tps)}

    barrier = pltpu.get_barrier_semaphore()

    @pl.loop(1, devices)
    def _(d):
        pl.semaphore_signal(barrier, inc=1, device_id=device_of(lax.rem(me + d, devices)), device_id_type=MESH)

    pl.semaphore_wait(barrier, devices - 1)

    for da, db in order:
        for k in range(pieces):
            i = slot(da, db)
            r = pl.multiple_of(first_row(1 - c, da, db) + k * ch, ch)
            remote(grad.at[pl.ds(r, ch)], peer.at[i, part(k)], peer_s, peer_r.at[i * pieces + k], partner).start()
    for copy in state_copies:
        copy.start()

    def chip_sum(da, db, k):
        i = slot(da, db)
        own_copy(da, db, k).wait()
        remote(peer.at[i, part(k)], peer.at[i, part(k)], peer_s, peer_r.at[i * pieces + k], partner).wait_recv()
        return own[i, part(k), :].astype(F32) + peer[i, part(k), :].astype(F32)

    def copy1(da, db, k):
        i = (da - 1) * n2 + db
        return remote(part1.at[i, part(k)], land1.at[i, part(k)], s1, r1.at[i * pieces + k], at(da, 0))

    def copy2(db, k):
        i = db - 1
        return remote(part2.at[i, part(k)], land2.at[i, part(k)], s2, r2.at[i * pieces + k], at(0, db))

    def send1(da, db, k):
        part1[(da - 1) * n2 + db, part(k), :] = chip_sum(da, db, k).astype(BF16)
        copy1(da, db, k).start()

    def sum1(db, k):
        value = chip_sum(0, db, k)
        for da in shifts1:
            copy1(da, db, k).wait_recv()
            value = value + land1[(da - 1) * n2 + db, part(k), :].astype(F32)
        return value

    for k in range(pieces):
        for da in shifts1:
            for db in shifts2:
                send1(da, db, k)
    for k in range(pieces):
        for da in shifts1:
            send1(da, 0, k)
        for db in shifts2:
            part2[db - 1, part(k), :] = sum1(db, k).astype(BF16)
            copy2(db, k).start()
    acc = jnp.zeros((8, width), F32)
    for k in range(pieces):
        value = sum1(0, k)
        for db in shifts2:
            copy2(db, k).wait_recv()
            value = value + land2[db - 1, part(k), :].astype(F32)
        total[part(k), :] = value
        value = value * value
        for r in range(0, ch, 8):
            acc = acc + value[r : r + 8, :]

    mine = acc[:, :128]
    for j in range(128, width, 128):
        mine = mine + acc[:, j : j + 128]
    squares[me] = jnp.sum(mine, axis=0, keepdims=True)

    @pl.loop(1, devices)
    def _(d):
        remote(squares.at[me], squares.at[me], ns, nr, device_of(lax.rem(me + d, devices))).start()

    others = squares.at[pl.ds(0, devices - 1)]
    everyone = remote(others, others, ns, nr, partner)
    for copy in state_copies:
        copy.wait()
    everyone.wait_recv()
    everyone.wait_send()
    norm2 = jnp.full((8, 128), jnp.sum(jnp.sum(squares[...], axis=0)), F32)
    entries = float(tps * ends * ys * 2 * rows * width)
    factor = jnp.minimum(F32(1.0), F32(math.sqrt(entries)) / (jnp.sqrt(norm2) + 1e-06))[:1, :1]

    my_row = first_row(c, 0, 0)

    def piece_of(da, db, k):
        return w_out.at[pl.ds(pl.multiple_of(first_row(c, da, db) + k * ch, ch), ch)]

    def copy_a(da, src, k):
        return remote(src, src, a_s, a_r.at[(da - 1) * pieces + k], at(da, 0))

    def copy_b(db, src, k):
        return remote(src, src, b_s, b_r.at[(db - 1) * pieces + k], at(0, db))

    def copy_f(da, db, src, k):
        return remote(src, src, f_s, f_r.at[((da - 1) * (n2 - 1) + db - 1) * pieces + k], at(0, db))

    def copy_p(src):
        return remote(src, src, p_s, p_r, partner)

    for k in range(pieces):
        @pl.loop(0, ch // 16)
        def _(g):
            at_row = pl.multiple_of(k * ch + g * 16, 16)
            here = pl.ds(at_row, 16)
            clipped = factor * total[here, :]
            m = 0.9 * st1[here, :] + 0.1 * clipped
            v = 0.999 * st2[here, :] + 0.001 * clipped * clipped
            update = m / (1.0 - 0.9**STEP) / (jnp.sqrt(v / (1.0 - 0.999**STEP)) + 1e-08)
            w = st0[here, :]
            w = w - 0.01 * (update + 0.1 * w)
            moment_out[here, :] = m
            second_out[here, :] = v
            master_out[here, :] = w
            w_out[pl.ds(pl.multiple_of(my_row + at_row, 16), 16), :] = w.astype(BF16)

        src = piece_of(0, 0, k)
        for da in shifts1:
            copy_a(da, src, k).start()
        for db in shifts2:
            copy_b(db, src, k).start()
        copy_p(src).start()

    for k in range(pieces):
        for da in shifts1:
            src = piece_of(n1 - da, 0, k)
            copy_a(da, src, k).wait_recv()
            for db in shifts2:
                copy_f(da, db, src, k).start()
            copy_p(src).start()
        for db in shifts2:
            src = piece_of(0, n2 - db, k)
            copy_b(db, src, k).wait_recv()
            copy_p(src).start()
    for k in range(pieces):
        for da in shifts1:
            for db in shifts2:
                src = piece_of(n1 - da, n2 - db, k)
                copy_f(da, db, src, k).wait_recv()
                copy_p(src).start()

    half = w_out.at[pl.ds(0, n1 * n2 * rows)]
    remote(half, half, p_s, p_r, partner).wait_recv()
    remote(half, half, p_s, p_r, partner).wait_send()
    remote(peer, peer, peer_s, peer_r.at[0], partner).wait_send()
    remote(part1, land1, s1, r1.at[0], partner).wait_send()
    remote(part2, land2, s2, r2.at[0], partner).wait_send()
    for sem, count, recv in ((a_s, n1 - 1, a_r), (b_s, n2 - 1, b_r), (f_s, (n1 - 1) * (n2 - 1), f_r)):
        ref = w_out.at[pl.ds(0, count * rows)]
        remote(ref, ref, sem, recv.at[0], partner).wait_send()
    if staged:
        final = pltpu.make_async_copy(w_out, w_hbm, w_sem)
        final.start()
        final.wait()


def put_out(*refs):
    count = len(refs) // 2
    sems = refs[-1]
    copies = [
        pltpu.make_async_copy(src, dst, sems.at[i])
        for i, (src, dst) in enumerate(zip(refs[:count], refs[count : 2 * count]))
    ]
    for copy in copies:
        copy.start()
    for copy in copies:
        copy.wait()


def per_device(mesh, grad, master, moment, second):
    ends, dps, tps = (mesh.shape[name] for name in ("ends", "dp", "tp"))
    ys = dps // 2
    rows_tp, width = grad.shape[2:]
    rows = rows_tp // (ends * dps)
    pieces = 4 if rows % 64 == 0 else 1
    n1, n2 = (ends, ys) if ends == ys else (ys, ends)
    blocks = n1 * n2
    devices = ends * dps * tps
    dma = lambda n: pltpu.SemaphoreType.DMA((n,))
    one = pltpu.SemaphoreType.DMA
    block = lambda n, dtype=BF16: pltpu.VMEM((n, rows, width), dtype)
    state = lambda: pltpu.VMEM((rows, width), F32)
    scratch = [
        block(blocks), block(blocks),
        block((n1 - 1) * n2), block((n1 - 1) * n2),
        block(n2 - 1), block(n2 - 1),
        state(), state(), state(), state(),
        pltpu.VMEM((devices, 1, 128), F32),
        dma(blocks * pieces), dma(3), one, dma(blocks * pieces),
        one, dma((n1 - 1) * n2 * pieces), one, dma((n2 - 1) * pieces),
        one, one,
        one, dma((n1 - 1) * pieces), one, dma((n2 - 1) * pieces),
        one, dma((n1 - 1) * (n2 - 1) * pieces),
        one, one,
    ]
    block_bytes = rows * width * 2
    staged = rows_tp * width * 2 > 8 << 20
    if staged:
        scratch += [pltpu.VMEM((rows_tp, width), BF16), one]
    limit = block_bytes * (2 * blocks + 2 * (n1 - 1) * n2 + 2 * (n2 - 1) + 8 + staged * ends * dps) + devices * 4096 + (3 << 20)
    stays = pl.BlockSpec(memory_space=pltpu.HBM)
    vmem = pl.BlockSpec(memory_space=pltpu.VMEM)
    vmem_any = pl.BlockSpec(memory_space=pl.ANY)
    results = pl.pallas_call(
        functools.partial(kernel, (ends, ys, tps, rows, width, pieces, staged)),
        out_shape=(
            (pltpu.HBM if staged else pltpu.VMEM)((rows_tp, width), BF16),
            pltpu.VMEM((rows, width), F32),
            pltpu.VMEM((rows, width), F32),
            pltpu.VMEM((rows, width), F32),
        ),
        in_specs=[stays] * 4,
        out_specs=(stays if staged else vmem,) + (vmem,) * 3,
        scratch_shapes=scratch,
        compiler_params=pltpu.CompilerParams(collective_id=0, has_side_effects=True, vmem_limit_bytes=limit),
        name="sum_update_gather",
    )(*(pltpu.with_memory_space_constraint(x, pltpu.HBM) for x in (grad[0, 0], master[0], moment[0], second[0])))
    first = 1 if staged else 0
    here = results[first:]
    out = pl.pallas_call(
        put_out,
        out_shape=tuple(pltpu.HBM(x.shape, x.dtype) for x in here),
        in_specs=[vmem_any] * len(here),
        out_specs=(stays,) * len(here),
        scratch_shapes=[dma(len(here))],
        compiler_params=pltpu.CompilerParams(vmem_limit_bytes=1 << 20),
        name="put_out",
    )(*(pltpu.with_memory_space_constraint(x, pltpu.VMEM) for x in here))
    weights, master_out, moment_out, second_out = tuple(results[:first]) + tuple(out)
    return (weights, master_out[None], moment_out[None], second_out[None])


def solution(mesh):
    rows = P("tp", ("ends", "dp"), None)
    return jax.shard_map(
        functools.partial(per_device, mesh),
        mesh=mesh,
        in_specs=(P("ends", "dp", "tp", None), rows, rows, rows),
        out_specs=(P("tp", None), rows, rows, rows),
        check_vma=False,
    )
```
